32 devices in a mesh: inl: 4 (over z), xln: 8 (over y, x, core).
Axes of the slice: x: 2, y: 2, z: 4, core: 2. Of those that a mesh axis runs over, the one named last changes fastest.
Arguments:
- noisy: float32 [128, 256, 512], P('inl', 'xln'), may hold values from -6 to 6
- bound: float32 [128, 256, 512], P('inl', 'xln'), may hold values from 0.05 to 0.5
Outputs:
- denoised: float32 [128, 256, 512], P('inl', 'xln')
- dual: float32 [3, 128, 256, 512], P(None, 'inl', 'xln')
- norms: float32 [2, 2], replicated
The draws below stay inside these ranges and needn't reach their ends.
All inputs are finite; a program needn't handle non-finite values.
Results may differ from the reference program's by a relative error of at most 0.0001.
Values sent between devices are 32-bit elements; how exact they have to be, the bound alone decides.
A program may use at most 64 MiB of HBM per device.

```python
import math
import jax
import jax.numpy as jnp
from jax import lax

NZ = 512
ITERS = 2
NI = 128
NX = 256


def levels(key, shape, cuts, least, high):
    def one(position, blocks):
        draws = jax.random.uniform(jax.random.fold_in(jax.random.fold_in(key, 6), position), (blocks,), jnp.float32, least / len(cuts), high / len(cuts))
        return jnp.repeat(jnp.exp(draws), shape[position] // blocks).reshape((-1,) + (1,) * (len(shape) - position - 1))

    gain = one(*cuts[0])
    for cut in cuts[1:]:
        gain = gain * one(*cut)
    return gain


def bell_draw(stream_key, extent, spread, most, split=(), held_as=jnp.bfloat16):
    gain = levels(stream_key, extent, split, -0.22, 0.18) if split else 1.0
    values = jax.random.normal(stream_key, extent, jnp.float32) * spread * gain
    return jnp.minimum(jnp.maximum(values, -most), most).astype(held_as)


def setup_inputs(seed: int = 0) -> dict:
    splits = jax.random.split(jax.random.key(seed), 3)
    return {
        "noisy": bell_draw(splits[0], (NI, NX, NZ), 1.0, 6.0, ((0, 4), (1, 8)), jnp.float32),
        "bound": jnp.clip(jnp.exp(math.log(0.5) - 2.3025851 * jax.random.uniform(splits[1], (NI, NX, NZ), jnp.float32) ** levels(splits[1], (NI, NX, NZ), ((0, 4), (1, 8)), -0.2, 0.2)), 0.05, 0.5),
    }


SIGMA = 0.28
TAU = 0.28

def forward(field, axis):
    first = lax.slice_in_dim(field, 0, 1, axis=axis)
    return jnp.concatenate([jnp.diff(field, axis=axis), jnp.zeros_like(first)], axis=axis)

def backward(field, axis):
    size = field.shape[axis]
    first = lax.slice_in_dim(field, 0, 1, axis=axis)
    earlier = jnp.concatenate([jnp.zeros_like(first), lax.slice_in_dim(field, 0, size - 1, axis=axis)], axis=axis)
    return field - earlier

def reference(noisy, bound):
    primal = noisy
    smooth = noisy
    dual_parts = [jnp.zeros_like(noisy) for axis in range(3)]
    rows = []
    for step in range(ITERS):
        fresh = [jnp.clip(dual_parts[axis] + SIGMA * forward(smooth, axis), -bound, bound) for axis in range(3)]
        diverge = backward(fresh[0], 0) + backward(fresh[1], 1) + backward(fresh[2], 2)
        updated = (primal + TAU * diverge + TAU * noisy) / (1.0 + TAU)
        primal_sum = jnp.sum((updated - primal) ** 2)
        dual_sum = jnp.sum((fresh[0] - dual_parts[0]) ** 2) + jnp.sum((fresh[1] - dual_parts[1]) ** 2) + jnp.sum((fresh[2] - dual_parts[2]) ** 2)
        rows.append(jnp.sqrt(jnp.stack([primal_sum, dual_sum])))
        smooth = 2.0 * updated - primal
        primal = updated
        dual_parts = fresh
    return (primal, jnp.stack(dual_parts), jnp.stack(rows))
```

```python
import functools

import jax
import jax.numpy as jnp
from jax import lax
from jax.experimental import pallas as pl
from jax.experimental.pallas import tpu as pltpu
from jax.sharding import PartitionSpec as P

SIGMA = 0.28
TAU = 0.28
GAIN = TAU / (1.0 + TAU)


def clip(value, limit):
    return jnp.minimum(jnp.maximum(value, -limit), limit)


def fold(square):
    rows, lanes = square.shape
    total = square[0:8]
    for at in range(8, rows, 8):
        total = total + square[at : at + 8]
    part = total[:, 0:128]
    for at in range(128, lanes, 128):
        part = part + total[:, at : at + 128]
    return part


def kernel(
    ni_dev, nx_dev,
    noisy, bound, out, dual, norms,
    n, b, v, step,
    nx_first, nx_last, bx_last, nx_next, nx_prev, bx_prev,
    vx_first, vx_last, vx_next, vx_prev, dx_prev, di_prev,
    mine, others_x, others_i,
    load_sem, send_sem, recv_sem, xs_sem, xr_sem, is_sem, ir_sem,
):
    ni, nx, nz = noisy.shape
    top, end = ni, ni + 1
    my_i, my_x = lax.axis_index("inl"), lax.axis_index("xln")

    loads = []

    def load(src, dst):
        copy = pltpu.make_async_copy(src, dst, load_sem.at[len(loads)])
        copy.start()
        loads.append(copy)

    load(noisy.at[pl.ds(ni - 1, 1)], n.at[pl.ds(top, 1)])
    load(bound.at[pl.ds(ni - 1, 1)], b.at[pl.ds(top, 1)])
    load(noisy.at[pl.ds(0, 1)], n.at[pl.ds(1, 1)])
    load(noisy.at[pl.ds(1, ni - 2)], n.at[pl.ds(2, ni - 2)])
    load(bound.at[pl.ds(0, ni - 1)], b.at[pl.ds(1, ni - 1)])

    barrier = pltpu.get_barrier_semaphore()
    for axis, me, count in (("inl", my_i, ni_dev), ("xln", my_x, nx_dev)):
        for k in range(1, count):
            pl.semaphore_signal(
                barrier, inc=1, device_id={axis: lax.rem(me + k, count)},
                device_id_type=pl.DeviceIdType.MESH,
            )
    pl.semaphore_wait(barrier, ni_dev + nx_dev - 2)

    sent = []

    def send(slot, src, dst, axis, forward):
        me, count = (my_i, ni_dev) if axis == "inl" else (my_x, nx_dev)
        target = lax.rem(me + (1 if forward else count - 1), count)
        copy = pltpu.make_async_remote_copy(
            src_ref=src, dst_ref=dst, send_sem=send_sem.at[slot], recv_sem=recv_sem.at[slot],
            device_id={axis: target}, device_id_type=pl.DeviceIdType.MESH,
        )
        not_last, not_first = me < count - 1, me > 0
        can_send, can_recv = (not_last, not_first) if forward else (not_first, not_last)

        @pl.when(can_send)
        def _():
            copy.start()

        sent.append((copy, can_send))

        def arrive(fill):
            @pl.when(can_recv)
            def _():
                copy.wait_recv()

            @pl.when(jnp.logical_not(can_recv))
            def _():
                fill()

        return arrive

    def setter(dst, src):
        def fill():
            dst[...] = src[...]

        return fill

    loads[0].wait()
    got_n_prev = send(0, n.at[top], n.at[0], "inl", True)
    loads[1].wait()
    got_b_prev = send(1, b.at[top], b.at[0], "inl", True)
    loads[2].wait()
    got_n_next = send(2, n.at[1], n.at[end], "inl", False)
    loads[3].wait()
    nx_last[...] = n[1:end, nx - 1, :]
    got_nx_prev = send(3, nx_last, nx_prev, "xln", True)
    nx_first[...] = n[1:end, 0, :]
    got_nx_next = send(5, nx_first, nx_next, "xln", False)
    loads[4].wait()
    bx_last[...] = b[1:end, nx - 1, :]
    got_bx_prev = send(4, bx_last, bx_prev, "xln", True)

    row = lax.broadcasted_iota(jnp.int32, (nx, nz), 0)
    lane = lax.broadcasted_iota(jnp.int32, (nx, nz), 1)
    first_row, last_row = row == 0, row == nx - 1
    first_lane, last_lane = lane == 0, lane == nz - 1

    step[...] = jnp.zeros_like(step)

    def pass_one(i, carry):
        here, limit = n[i + 1], b[i + 1]
        di = clip(SIGMA * (n[i + 2] - here), limit)
        dx = clip(SIGMA * jnp.where(last_row, 0.0, pltpu.roll(here, nx - 1, 0) - here), limit)
        dz = clip(SIGMA * jnp.where(last_lane, 0.0, pltpu.roll(here, nz - 1, 1) - here), limit)
        dual[0, i] = di
        dual[1, i] = dx
        dual[2, i] = dz
        div = di - step[...]
        div = div + (dx - jnp.where(first_row, 0.0, pltpu.roll(dx, 1, 0)))
        div = div + (dz - jnp.where(first_lane, 0.0, pltpu.roll(dz, 1, 1)))
        step[...] = di
        v[i + 1] = here + (2.0 * GAIN) * div
        return carry

    lax.fori_loop(0, ni - 1, pass_one, 0)
    here, limit = n[top], b[top]
    dx = clip(SIGMA * jnp.where(last_row, 0.0, pltpu.roll(here, nx - 1, 0) - here), limit)
    dz = clip(SIGMA * jnp.where(last_lane, 0.0, pltpu.roll(here, nz - 1, 1) - here), limit)
    dual[1, ni - 1] = dx
    dual[2, ni - 1] = dz
    div = (dx - jnp.where(first_row, 0.0, pltpu.roll(dx, 1, 0))) - step[...]
    div = div + (dz - jnp.where(first_lane, 0.0, pltpu.roll(dz, 1, 1)))
    v[top] = here + (2.0 * GAIN) * div

    got_nx_prev(setter(nx_prev, nx_first))
    got_bx_prev(setter(bx_prev, bx_last))
    got_nx_next(setter(nx_next, nx_last))
    dx_last = clip(SIGMA * (nx_next[...] - nx_last[...]), bx_last[...])
    dxp = clip(SIGMA * (nx_first[...] - nx_prev[...]), bx_prev[...])
    dual[1, :, nx - 1, :] = dx_last
    dx_prev[...] = dxp
    v[1:end, nx - 1, :] = v[1:end, nx - 1, :] + (2.0 * GAIN) * dx_last
    v[1:end, 0, :] = v[1:end, 0, :] - (2.0 * GAIN) * dxp

    got_n_prev(setter(n.at[0], n.at[1]))
    got_b_prev(setter(b.at[0], b.at[1]))
    got_n_next(setter(n.at[end], n.at[top]))
    di_last = clip(SIGMA * (n[end] - n[top]), b[top])
    dip = clip(SIGMA * (n[1] - n[0]), b[0])
    dual[0, ni - 1] = di_last
    di_prev[...] = dip
    v[top] = v[top] + (2.0 * GAIN) * di_last
    v[1] = v[1] - (2.0 * GAIN) * dip

    got_v_prev = send(6, v.at[top], v.at[0], "inl", True)
    got_v_next = send(7, v.at[1], v.at[end], "inl", False)
    vx_last[...] = v[1:end, nx - 1, :]
    got_vx_prev = send(8, vx_last, vx_prev, "xln", True)
    vx_first[...] = v[1:end, 0, :]
    got_vx_next = send(9, vx_first, vx_next, "xln", False)

    got_vx_prev(setter(vx_prev, vx_first))
    got_vx_next(setter(vx_next, vx_last))
    got_v_prev(setter(v.at[0], v.at[1]))
    got_v_next(setter(v.at[end], v.at[top]))
    dx_prev[...] = clip(dx_prev[...] + SIGMA * (vx_first[...] - vx_prev[...]), bx_prev[...])
    step[...] = clip(di_prev[...] + SIGMA * (v[1] - v[0]), b[0])

    def pass_two(i, sums):
        p1, d1, p2, d2 = sums
        here, limit, base = v[i + 1], b[i + 1], n[i + 1]
        oi, ox, oz = dual[0, i], dual[1, i], dual[2, i]
        di = clip(oi + SIGMA * (v[i + 2] - here), limit)
        ahead = jnp.where(last_row, vx_next[pl.ds(i, 1), :], pltpu.roll(here, nx - 1, 0))
        dx = clip(ox + SIGMA * (ahead - here), limit)
        dz = clip(
            oz + SIGMA * jnp.where(last_lane, 0.0, pltpu.roll(here, nz - 1, 1) - here), limit
        )
        dual[0, i] = di
        dual[1, i] = dx
        dual[2, i] = dz
        div = di - step[...]
        div = div + (dx - jnp.where(first_row, dx_prev[pl.ds(i, 1), :], pltpu.roll(dx, 1, 0)))
        div = div + (dz - jnp.where(first_lane, 0.0, pltpu.roll(dz, 1, 1)))
        step[...] = di
        half = 0.5 * (here - base)
        change = GAIN * (div - half)
        out[i] = base + half + change
        p1 = p1 + fold(half * half)
        d1 = d1 + fold(oi * oi + ox * ox + oz * oz)
        p2 = p2 + fold(change * change)
        oi, ox, oz = di - oi, dx - ox, dz - oz
        d2 = d2 + fold(oi * oi + ox * ox + oz * oz)
        return p1, d1, p2, d2

    zero = jnp.zeros((8, 128), jnp.float32)
    sums = lax.fori_loop(0, ni, pass_two, (zero,) * 4)

    for k in range(4):
        mine[0, k] = sums[k]

    def reduce(count, me, axis, source, others, ss, rs):
        copies = []
        for k in range(1, count):
            copy = pltpu.make_async_remote_copy(
                src_ref=source, dst_ref=others.at[k - 1],
                send_sem=ss.at[k - 1], recv_sem=rs.at[k - 1],
                device_id={axis: lax.rem(me + k, count)}, device_id_type=pl.DeviceIdType.MESH,
            )
            copy.start()
            copies.append(copy)
        total = source[...]
        for copy in copies:
            copy.wait_recv()
        for k in range(count - 1):
            total = total + others[k]
        return total, copies

    total, copies_x = reduce(nx_dev, my_x, "xln", mine.at[0], others_x, xs_sem, xr_sem)
    mine[1] = total
    total, copies_i = reduce(ni_dev, my_i, "inl", mine.at[1], others_i, is_sem, ir_sem)
    at = 2 * lax.broadcasted_iota(jnp.int32, (2, 2), 0) + lax.broadcasted_iota(jnp.int32, (2, 2), 1)
    result = jnp.zeros((2, 2), jnp.float32)
    for k in range(4):
        result = jnp.where(at == k, jnp.sum(total[k]), result)
    norms[...] = jnp.sqrt(result)

    for copy in copies_x + copies_i:
        copy.wait_send()
    for copy, can_send in sent:
        @pl.when(can_send)
        def _():
            copy.wait_send()


def per_device(noisy, bound):
    ni, nx, nz = noisy.shape
    ni_dev, nx_dev = lax.axis_size("inl"), lax.axis_size("xln")
    f32 = jnp.float32
    face = pltpu.VMEM((ni, nz), f32)
    slab = pltpu.VMEM((nx, nz), f32)
    dma = pltpu.SemaphoreType.DMA
    volume = 4 * ni * nx * nz
    return pl.pallas_call(
        functools.partial(kernel, ni_dev, nx_dev),
        out_shape=(
            pltpu.VMEM((ni, nx, nz), f32),
            pltpu.VMEM((3, ni, nx, nz), f32),
            jax.ShapeDtypeStruct((2, 2), f32),
        ),
        in_specs=[pl.BlockSpec(memory_space=pltpu.HBM)] * 2,
        out_specs=(
            pl.BlockSpec(memory_space=pltpu.VMEM),
            pl.BlockSpec(memory_space=pltpu.VMEM),
            pl.BlockSpec(memory_space=pltpu.VMEM),
        ),
        scratch_shapes=[
            pltpu.VMEM((ni + 2, nx, nz), f32),
            pltpu.VMEM((ni + 1, nx, nz), f32),
            pltpu.VMEM((ni + 2, nx, nz), f32),
            slab,
            *([face] * 11),
            slab,
            pltpu.VMEM((2, 4, 8, 128), f32),
            pltpu.VMEM((nx_dev - 1, 4, 8, 128), f32),
            pltpu.VMEM((ni_dev - 1, 4, 8, 128), f32),
            dma((5,)), dma((10,)), dma((10,)),
            dma((nx_dev - 1,)), dma((nx_dev - 1,)), dma((ni_dev - 1,)), dma((ni_dev - 1,)),
        ],
        compiler_params=pltpu.CompilerParams(
            collective_id=0, has_side_effects=True, vmem_limit_bytes=24 * 1024 * 1024
        ),
        cost_estimate=pl.CostEstimate(
            flops=80 * ni * nx * nz, bytes_accessed=6 * volume, transcendentals=0
        ),
        name="denoise",
    )(noisy, bound)


def solution(mesh):
    in_specs = (P("inl", "xln", None), P("inl", "xln", None))
    out_specs = (P("inl", "xln", None), P(None, "inl", "xln", None), P())
    return jax.shard_map(
        per_device, mesh=mesh, in_specs=in_specs, out_specs=out_specs, check_vma=False
    )
```

```python
import functools

import jax
import jax.numpy as jnp
from jax import lax
from jax.experimental import pallas as pl
from jax.experimental.pallas import tpu as pltpu
from jax.sharding import PartitionSpec as P

SIGMA = 0.28
TAU = 0.28
GAIN = TAU / (1.0 + TAU)


def clip(value, limit):
    return jnp.minimum(jnp.maximum(value, -limit), limit)


def fold(square):
    rows, lanes = square.shape
    total = square[0:8]
    for at in range(8, rows, 8):
        total = total + square[at : at + 8]
    part = total[:, 0:128]
    for at in range(128, lanes, 128):
        part = part + total[:, at : at + 128]
    return part


def kernel(
    ni_dev, nx_dev,
    noisy, bound, out, dual, norms,
    n, b, v, step,
    nx_first, nx_last, bx_last, nx_next, nx_prev, bx_prev,
    vx_first, vx_last, vx_next, vx_prev, dx_prev, di_prev,
    mine, others_x, others_i,
    load_sem, send_sem, recv_sem, xs_sem, xr_sem, is_sem, ir_sem,
):
    ni, nx, nz = noisy.shape
    top, end = ni, ni + 1
    my_i, my_x = lax.axis_index("inl"), lax.axis_index("xln")

    loads = []

    def load(src, dst):
        copy = pltpu.make_async_copy(src, dst, load_sem.at[len(loads)])
        copy.start()
        loads.append(copy)

    load(noisy.at[pl.ds(ni - 1, 1)], n.at[pl.ds(top, 1)])
    load(bound.at[pl.ds(ni - 1, 1)], b.at[pl.ds(top, 1)])
    load(noisy.at[pl.ds(0, 1)], n.at[pl.ds(1, 1)])
    load(noisy.at[pl.ds(1, ni - 2)], n.at[pl.ds(2, ni - 2)])
    load(bound.at[pl.ds(0, ni - 1)], b.at[pl.ds(1, ni - 1)])

    barrier = pltpu.get_barrier_semaphore()
    for axis, me, count in (("inl", my_i, ni_dev), ("xln", my_x, nx_dev)):
        for k in range(1, count):
            pl.semaphore_signal(
                barrier, inc=1, device_id={axis: lax.rem(me + k, count)},
                device_id_type=pl.DeviceIdType.MESH,
            )
    pl.semaphore_wait(barrier, ni_dev + nx_dev - 2)

    sent = []

    def send(slot, src, dst, axis, forward):
        me, count = (my_i, ni_dev) if axis == "inl" else (my_x, nx_dev)
        target = lax.rem(me + (1 if forward else count - 1), count)
        copy = pltpu.make_async_remote_copy(
            src_ref=src, dst_ref=dst, send_sem=send_sem.at[slot], recv_sem=recv_sem.at[slot],
            device_id={axis: target}, device_id_type=pl.DeviceIdType.MESH,
        )
        not_last, not_first = me < count - 1, me > 0
        can_send, can_recv = (not_last, not_first) if forward else (not_first, not_last)

        @pl.when(can_send)
        def _():
            copy.start()

        sent.append((copy, can_send))

        def arrive(fill):
            @pl.when(can_recv)
            def _():
                copy.wait_recv()

            @pl.when(jnp.logical_not(can_recv))
            def _():
                fill()

        return arrive

    def setter(dst, src):
        def fill():
            dst[...] = src[...]

        return fill

    loads[0].wait()
    got_n_prev = send(0, n.at[top], n.at[0], "inl", True)
    loads[1].wait()
    got_b_prev = send(1, b.at[top], b.at[0], "inl", True)
    loads[2].wait()
    got_n_next = send(2, n.at[1], n.at[end], "inl", False)
    loads[3].wait()
    nx_last[...] = n[1:end, nx - 1, :]
    got_nx_prev = send(3, nx_last, nx_prev, "xln", True)
    nx_first[...] = n[1:end, 0, :]
    got_nx_next = send(5, nx_first, nx_next, "xln", False)
    loads[4].wait()
    bx_last[...] = b[1:end, nx - 1, :]
    got_bx_prev = send(4, bx_last, bx_prev, "xln", True)

    row = lax.broadcasted_iota(jnp.int32, (nx, nz), 0)
    lane = lax.broadcasted_iota(jnp.int32, (nx, nz), 1)
    first_row, last_row = row == 0, row == nx - 1
    first_lane, last_lane = lane == 0, lane == nz - 1

    step[...] = jnp.zeros_like(step)

    def pass_one(i, carry):
        here, limit = n[i + 1], b[i + 1]
        di = clip(SIGMA * (n[i + 2] - here), limit)
        dx = clip(SIGMA * jnp.where(last_row, 0.0, pltpu.roll(here, nx - 1, 0) - here), limit)
        dz = clip(SIGMA * jnp.where(last_lane, 0.0, pltpu.roll(here, nz - 1, 1) - here), limit)
        dual[0, i] = di
        dual[1, i] = dx
        dual[2, i] = dz
        div = di - step[...]
        div = div + (dx - jnp.where(first_row, 0.0, pltpu.roll(dx, 1, 0)))
        div = div + (dz - jnp.where(first_lane, 0.0, pltpu.roll(dz, 1, 1)))
        step[...] = di
        v[i + 1] = here + (2.0 * GAIN) * div
        return carry

    lax.fori_loop(0, ni - 1, pass_one, 0)
    here, limit = n[top], b[top]
    dx = clip(SIGMA * jnp.where(last_row, 0.0, pltpu.roll(here, nx - 1, 0) - here), limit)
    dz = clip(SIGMA * jnp.where(last_lane, 0.0, pltpu.roll(here, nz - 1, 1) - here), limit)
    dual[1, ni - 1] = dx
    dual[2, ni - 1] = dz
    div = (dx - jnp.where(first_row, 0.0, pltpu.roll(dx, 1, 0))) - step[...]
    div = div + (dz - jnp.where(first_lane, 0.0, pltpu.roll(dz, 1, 1)))
    v[top] = here + (2.0 * GAIN) * div

    got_nx_prev(setter(nx_prev, nx_first))
    got_bx_prev(setter(bx_prev, bx_last))
    got_nx_next(setter(nx_next, nx_last))
    dx_last = clip(SIGMA * (nx_next[...] - nx_last[...]), bx_last[...])
    dxp = clip(SIGMA * (nx_first[...] - nx_prev[...]), bx_prev[...])
    dual[1, :, nx - 1, :] = dx_last
    dx_prev[...] = dxp
    v[1:end, nx - 1, :] = v[1:end, nx - 1, :] + (2.0 * GAIN) * dx_last
    v[1:end, 0, :] = v[1:end, 0, :] - (2.0 * GAIN) * dxp

    got_n_prev(setter(n.at[0], n.at[1]))
    got_b_prev(setter(b.at[0], b.at[1]))
    got_n_next(setter(n.at[end], n.at[top]))
    di_last = clip(SIGMA * (n[end] - n[top]), b[top])
    dip = clip(SIGMA * (n[1] - n[0]), b[0])
    dual[0, ni - 1] = di_last
    di_prev[...] = dip
    v[top] = v[top] + (2.0 * GAIN) * di_last
    v[1] = v[1] - (2.0 * GAIN) * dip

    got_v_prev = send(6, v.at[top], v.at[0], "inl", True)
    got_v_next = send(7, v.at[1], v.at[end], "inl", False)
    vx_last[...] = v[1:end, nx - 1, :]
    got_vx_prev = send(8, vx_last, vx_prev, "xln", True)
    vx_first[...] = v[1:end, 0, :]
    got_vx_next = send(9, vx_first, vx_next, "xln", False)

    got_vx_prev(setter(vx_prev, vx_first))
    got_vx_next(setter(vx_next, vx_last))
    got_v_prev(setter(v.at[0], v.at[1]))
    got_v_next(setter(v.at[end], v.at[top]))
    dx_prev[...] = clip(dx_prev[...] + SIGMA * (vx_first[...] - vx_prev[...]), bx_prev[...])
    step[...] = clip(di_prev[...] + SIGMA * (v[1] - v[0]), b[0])

    def pass_two(i, sums):
        p1, d1, p2, d2 = sums
        here, limit, base = v[i + 1], b[i + 1], n[i + 1]
        oi, ox, oz = dual[0, i], dual[1, i], dual[2, i]
        di = clip(oi + SIGMA * (v[i + 2] - here), limit)
        ahead = jnp.where(last_row, vx_next[pl.ds(i, 1), :], pltpu.roll(here, nx - 1, 0))
        dx = clip(ox + SIGMA * (ahead - here), limit)
        dz = clip(
            oz + SIGMA * jnp.where(last_lane, 0.0, pltpu.roll(here, nz - 1, 1) - here), limit
        )
        dual[0, i] = di
        dual[1, i] = dx
        dual[2, i] = dz
        div = di - step[...]
        div = div + (dx - jnp.where(first_row, dx_prev[pl.ds(i, 1), :], pltpu.roll(dx, 1, 0)))
        div = div + (dz - jnp.where(first_lane, 0.0, pltpu.roll(dz, 1, 1)))
        step[...] = di
        half = 0.5 * (here - base)
        change = GAIN * (div - half)
        out[i] = base + half + change
        p1 = p1 + fold(half * half)
        d1 = d1 + fold(oi * oi + ox * ox + oz * oz)
        p2 = p2 + fold(change * change)
        oi, ox, oz = di - oi, dx - ox, dz - oz
        d2 = d2 + fold(oi * oi + ox * ox + oz * oz)
        return p1, d1, p2, d2

    zero = jnp.zeros((8, 128), jnp.float32)
    sums = lax.fori_loop(0, ni, pass_two, (zero,) * 4)

    for k in range(4):
        mine[0, k] = sums[k]

    def reduce(count, me, axis, source, others, ss, rs):
        copies = []
        for k in range(1, count):
            copy = pltpu.make_async_remote_copy(
                src_ref=source, dst_ref=others.at[k - 1],
                send_sem=ss.at[k - 1], recv_sem=rs.at[k - 1],
                device_id={axis: lax.rem(me + k, count)}, device_id_type=pl.DeviceIdType.MESH,
            )
            copy.start()
            copies.append(copy)
        total = source[...]
        for copy in copies:
            copy.wait_recv()
        for k in range(count - 1):
            total = total + others[k]
        return total, copies

    total, copies_x = reduce(nx_dev, my_x, "xln", mine.at[0], others_x, xs_sem, xr_sem)
    mine[1] = total
    total, copies_i = reduce(ni_dev, my_i, "inl", mine.at[1], others_i, is_sem, ir_sem)
    at = 2 * lax.broadcasted_iota(jnp.int32, (2, 2), 0) + lax.broadcasted_iota(jnp.int32, (2, 2), 1)
    result = jnp.zeros((2, 2), jnp.float32)
    for k in range(4):
        result = jnp.where(at == k, jnp.sum(total[k]), result)
    norms[...] = jnp.sqrt(result)

    for copy in copies_x + copies_i:
        copy.wait_send()
    for copy, can_send in sent:
        @pl.when(can_send)
        def _():
            copy.wait_send()


def put_out(out_held, dual_held, norms_held, out, dual, norms, sems):
    half = out.shape[0] // 2
    pairs = [(norms_held, norms)]
    for at in (0, half):
        part = pl.ds(at, half)
        pairs.append((out_held.at[part], out.at[part]))
        for axis in range(3):
            pairs.append((dual_held.at[axis, part], dual.at[axis, part]))
    copies = [pltpu.make_async_copy(src, dst, sems.at[k]) for k, (src, dst) in enumerate(pairs)]
    for copy in copies:
        copy.start()
    for copy in copies:
        copy.wait()


def per_device(noisy, bound):
    ni, nx, nz = noisy.shape
    ni_dev, nx_dev = lax.axis_size("inl"), lax.axis_size("xln")
    f32 = jnp.float32
    face = pltpu.VMEM((ni, nz), f32)
    slab = pltpu.VMEM((nx, nz), f32)
    dma = pltpu.SemaphoreType.DMA
    volume = 4 * ni * nx * nz
    noisy = pltpu.with_memory_space_constraint(noisy, pltpu.HBM)
    bound = pltpu.with_memory_space_constraint(bound, pltpu.HBM)
    held = pl.pallas_call(
        functools.partial(kernel, ni_dev, nx_dev),
        out_shape=(
            pltpu.VMEM((ni, nx, nz), f32),
            pltpu.VMEM((3, ni, nx, nz), f32),
            pltpu.VMEM((2, 2), f32),
        ),
        in_specs=[pl.BlockSpec(memory_space=pltpu.HBM)] * 2,
        out_specs=(
            pl.BlockSpec(memory_space=pltpu.VMEM),
            pl.BlockSpec(memory_space=pltpu.VMEM),
            pl.BlockSpec(memory_space=pltpu.VMEM),
        ),
        scratch_shapes=[
            pltpu.VMEM((ni + 2, nx, nz), f32),
            pltpu.VMEM((ni + 1, nx, nz), f32),
            pltpu.VMEM((ni + 2, nx, nz), f32),
            slab,
            *([face] * 11),
            slab,
            pltpu.VMEM((2, 4, 8, 128), f32),
            pltpu.VMEM((nx_dev - 1, 4, 8, 128), f32),
            pltpu.VMEM((ni_dev - 1, 4, 8, 128), f32),
            dma((5,)), dma((10,)), dma((10,)),
            dma((nx_dev - 1,)), dma((nx_dev - 1,)), dma((ni_dev - 1,)), dma((ni_dev - 1,)),
        ],
        compiler_params=pltpu.CompilerParams(
            collective_id=0, has_side_effects=True, vmem_limit_bytes=24 * 1024 * 1024
        ),
        cost_estimate=pl.CostEstimate(
            flops=80 * ni * nx * nz, bytes_accessed=6 * volume, transcendentals=0
        ),
        name="denoise",
    )(noisy, bound)
    in_vmem = pl.BlockSpec(memory_space=pltpu.VMEM)
    in_hbm = pl.BlockSpec(memory_space=pltpu.HBM)
    return pl.pallas_call(
        put_out,
        out_shape=(
            jax.ShapeDtypeStruct((ni, nx, nz), f32),
            jax.ShapeDtypeStruct((3, ni, nx, nz), f32),
            jax.ShapeDtypeStruct((2, 2), f32),
        ),
        in_specs=[in_vmem] * 3,
        out_specs=(in_hbm,) * 3,
        scratch_shapes=[dma((9,))],
        compiler_params=pltpu.CompilerParams(vmem_limit_bytes=1024 * 1024),
        cost_estimate=pl.CostEstimate(flops=0, bytes_accessed=4 * volume, transcendentals=0),
        name="put_out",
    )(*held)


def solution(mesh):
    in_specs = (P("inl", "xln", None), P("inl", "xln", None))
    out_specs = (P("inl", "xln", None), P(None, "inl", "xln", None), P())
    return jax.shard_map(
        per_device, mesh=mesh, in_specs=in_specs, out_specs=out_specs, check_vma=False
    )
```

```python
import functools

import jax
import jax.numpy as jnp
from jax import lax
from jax.experimental import pallas as pl
from jax.experimental.pallas import tpu as pltpu
from jax.sharding import PartitionSpec as P

SIGMA = 0.28
TAU = 0.28
GAIN = TAU / (1.0 + TAU)


def clip(value, limit):
    return jnp.minimum(jnp.maximum(value, -limit), limit)


def fold(square):
    rows, lanes = square.shape
    total = square[0:8]
    for at in range(8, rows, 8):
        total = total + square[at : at + 8]
    part = total[:, 0:128]
    for at in range(128, lanes, 128):
        part = part + total[:, at : at + 128]
    return part


def kernel(
    ni_dev, nx_dev,
    noisy, bound, out, dual, norms,
    n, b, v, step,
    nx_first, nx_last, bx_last, nx_next, nx_prev, bx_prev,
    vx_first, vx_last, vx_next, vx_prev, dx_prev, dx_edge, di_prev,
    mine, others_x, others_i,
    load_sem, send_sem, recv_sem, xs_sem, xr_sem, is_sem, ir_sem,
):
    ni, nx, nz = noisy.shape
    top, end = ni, ni + 1
    my_i, my_x = lax.axis_index("inl"), lax.axis_index("xln")

    loads = []

    def load(src, dst):
        copy = pltpu.make_async_copy(src, dst, load_sem.at[len(loads)])
        copy.start()
        loads.append(copy)

    load(noisy.at[pl.ds(ni - 1, 1)], n.at[pl.ds(top, 1)])
    load(bound.at[pl.ds(ni - 1, 1)], b.at[pl.ds(top, 1)])
    load(noisy.at[pl.ds(0, 1)], n.at[pl.ds(1, 1)])
    load(noisy.at[pl.ds(1, ni - 2)], n.at[pl.ds(2, ni - 2)])
    load(bound.at[pl.ds(0, ni - 1)], b.at[pl.ds(1, ni - 1)])

    barrier = pltpu.get_barrier_semaphore()
    for axis, me, count in (("inl", my_i, ni_dev), ("xln", my_x, nx_dev)):
        for k in range(1, count):
            pl.semaphore_signal(
                barrier, inc=1, device_id={axis: lax.rem(me + k, count)},
                device_id_type=pl.DeviceIdType.MESH,
            )
    pl.semaphore_wait(barrier, ni_dev + nx_dev - 2)

    sent = []

    def send(slot, src, dst, axis, forward):
        me, count = (my_i, ni_dev) if axis == "inl" else (my_x, nx_dev)
        target = lax.rem(me + (1 if forward else count - 1), count)
        copy = pltpu.make_async_remote_copy(
            src_ref=src, dst_ref=dst, send_sem=send_sem.at[slot], recv_sem=recv_sem.at[slot],
            device_id={axis: target}, device_id_type=pl.DeviceIdType.MESH,
        )
        not_last, not_first = me < count - 1, me > 0
        can_send, can_recv = (not_last, not_first) if forward else (not_first, not_last)

        @pl.when(can_send)
        def _():
            copy.start()

        sent.append((copy, can_send))

        def arrive(fill):
            @pl.when(can_recv)
            def _():
                copy.wait_recv()

            @pl.when(jnp.logical_not(can_recv))
            def _():
                fill()

        return arrive

    def setter(dst, src):
        def fill():
            dst[...] = src[...]

        return fill

    loads[0].wait()
    got_n_prev = send(0, n.at[top], n.at[0], "inl", True)
    loads[1].wait()
    got_b_prev = send(1, b.at[top], b.at[0], "inl", True)
    loads[2].wait()
    got_n_next = send(2, n.at[1], n.at[end], "inl", False)
    loads[3].wait()
    nx_last[...] = n[1:end, nx - 1, :]
    got_nx_prev = send(3, nx_last, nx_prev, "xln", True)
    nx_first[...] = n[1:end, 0, :]
    got_nx_next = send(5, nx_first, nx_next, "xln", False)
    loads[4].wait()
    bx_last[...] = b[1:end, nx - 1, :]
    got_bx_prev = send(4, bx_last, bx_prev, "xln", True)

    row = lax.broadcasted_iota(jnp.int32, (nx, nz), 0)
    lane = lax.broadcasted_iota(jnp.int32, (nx, nz), 1)
    first_row, last_row = row == 0, row == nx - 1
    first_lane, last_lane = lane == 0, lane == nz - 1

    step[...] = jnp.zeros_like(step)

    def squares(oi, ox, oz):
        return fold(oi * oi + ox * ox + oz * oz)

    def pass_one(i, d1):
        here, limit = n[i + 1], b[i + 1]
        di = clip(SIGMA * (n[i + 2] - here), limit)
        dx = clip(SIGMA * jnp.where(last_row, 0.0, pltpu.roll(here, nx - 1, 0) - here), limit)
        dz = clip(SIGMA * jnp.where(last_lane, 0.0, pltpu.roll(here, nz - 1, 1) - here), limit)
        dual[0, i] = di
        dual[1, i] = dx
        dual[2, i] = dz
        div = di - step[...]
        div = div + (dx - jnp.where(first_row, 0.0, pltpu.roll(dx, 1, 0)))
        div = div + (dz - jnp.where(first_lane, 0.0, pltpu.roll(dz, 1, 1)))
        step[...] = di
        v[i + 1] = here + (2.0 * GAIN) * div
        return d1 + squares(di, dx, dz)

    zero = jnp.zeros((8, 128), jnp.float32)
    d1 = lax.fori_loop(0, ni - 1, pass_one, zero)
    here, limit = n[top], b[top]
    dx = clip(SIGMA * jnp.where(last_row, 0.0, pltpu.roll(here, nx - 1, 0) - here), limit)
    dz = clip(SIGMA * jnp.where(last_lane, 0.0, pltpu.roll(here, nz - 1, 1) - here), limit)
    dual[1, ni - 1] = dx
    dual[2, ni - 1] = dz
    div = (dx - jnp.where(first_row, 0.0, pltpu.roll(dx, 1, 0))) - step[...]
    div = div + (dz - jnp.where(first_lane, 0.0, pltpu.roll(dz, 1, 1)))
    v[top] = here + (2.0 * GAIN) * div
    d1 = d1 + fold(dx * dx + dz * dz)

    got_nx_prev(setter(nx_prev, nx_first))
    got_bx_prev(setter(bx_prev, bx_last))
    got_nx_next(setter(nx_next, nx_last))
    dx_last = clip(SIGMA * (nx_next[...] - nx_last[...]), bx_last[...])
    dxp = clip(SIGMA * (nx_first[...] - nx_prev[...]), bx_prev[...])
    dual[1, :, nx - 1, :] = dx_last
    dx_prev[...] = dxp
    dx_edge[...] = dx_last
    v[1:end, nx - 1, :] = v[1:end, nx - 1, :] + (2.0 * GAIN) * dx_last
    v[1:end, 0, :] = v[1:end, 0, :] - (2.0 * GAIN) * dxp

    got_n_prev(setter(n.at[0], n.at[1]))
    got_b_prev(setter(b.at[0], b.at[1]))
    got_n_next(setter(n.at[end], n.at[top]))
    di_last = clip(SIGMA * (n[end] - n[top]), b[top])
    dip = clip(SIGMA * (n[1] - n[0]), b[0])
    dual[0, ni - 1] = di_last
    di_prev[...] = dip
    v[top] = v[top] + (2.0 * GAIN) * di_last
    v[1] = v[1] - (2.0 * GAIN) * dip
    got_v_prev = send(6, v.at[top], v.at[0], "inl", True)
    got_v_next = send(7, v.at[1], v.at[end], "inl", False)
    vx_last[...] = v[1:end, nx - 1, :]
    got_vx_prev = send(8, vx_last, vx_prev, "xln", True)
    vx_first[...] = v[1:end, 0, :]
    got_vx_next = send(9, vx_first, vx_next, "xln", False)
    d1 = d1 + fold(di_last * di_last) + fold(dx_last * dx_last)

    face_row = first_row | last_row

    def pass_two(i, sums):
        p1, p2, d2 = sums
        here, limit, base = v[i + 1], b[i + 1], n[i + 1]
        oi, ox, oz = dual[0, i], dual[1, i], dual[2, i]
        di = clip(oi + SIGMA * (v[i + 2] - here), limit)
        ahead = jnp.where(last_row, 0.0, pltpu.roll(here, nx - 1, 0) - here)
        dx = clip(ox + SIGMA * ahead, limit)
        ahead = jnp.where(last_lane, 0.0, pltpu.roll(here, nz - 1, 1) - here)
        dz = clip(oz + SIGMA * ahead, limit)
        dual[0, i] = di
        dual[1, i] = dx
        dual[2, i] = dz
        div = di - step[...]
        div = div + (dx - jnp.where(first_row, 0.0, pltpu.roll(dx, 1, 0)))
        div = div + (dz - jnp.where(first_lane, 0.0, pltpu.roll(dz, 1, 1)))
        step[...] = di
        half = 0.5 * (here - base)
        change = GAIN * (div - half)
        out[i] = base + half + change
        inner = jnp.where(face_row, 0.0, change)
        return (
            p1 + fold(half * half),
            p2 + fold(inner * inner),
            d2 + squares(di - oi, dx - ox, dz - oz),
        )

    step[...] = clip(dual[0, 0] + SIGMA * (v[2] - v[1]), b[1])
    sums = lax.fori_loop(1, ni - 1, pass_two, (zero,) * 3)

    got_v_next(setter(v.at[end], v.at[top]))
    sums = pass_two(ni - 1, sums)
    got_v_prev(setter(v.at[0], v.at[1]))
    step[...] = clip(di_prev[...] + SIGMA * (v[1] - v[0]), b[0])
    p1, p2, d2 = pass_two(0, sums)

    got_vx_prev(setter(vx_prev, vx_first))
    got_vx_next(setter(vx_next, vx_last))
    was = dx_edge[...]
    dx_last = clip(was + SIGMA * (vx_next[...] - vx_last[...]), bx_last[...])
    dual[1, :, nx - 1, :] = dx_last
    moved = dx_last - was
    d2 = d2 + fold(moved * moved)
    u_last = out[:, nx - 1, :] + GAIN * moved
    out[:, nx - 1, :] = u_last
    dxp = clip(dx_prev[...] + SIGMA * (vx_first[...] - vx_prev[...]), bx_prev[...])
    u_first = out[:, 0, :] - GAIN * dxp
    out[:, 0, :] = u_first
    change = u_last - (nx_last[...] + 0.5 * (vx_last[...] - nx_last[...]))
    p2 = p2 + fold(change * change)
    change = u_first - (nx_first[...] + 0.5 * (vx_first[...] - nx_first[...]))
    p2 = p2 + fold(change * change)

    for k, part in enumerate((p1, d1, p2, d2)):
        mine[0, k : k + 1] = jnp.sum(part, axis=0, keepdims=True)

    def reduce(count, me, axis, source, others, ss, rs):
        copies = []
        for k in range(1, count):
            copy = pltpu.make_async_remote_copy(
                src_ref=source, dst_ref=others.at[k - 1],
                send_sem=ss.at[k - 1], recv_sem=rs.at[k - 1],
                device_id={axis: lax.rem(me + k, count)}, device_id_type=pl.DeviceIdType.MESH,
            )
            copy.start()
            copies.append(copy)
        total = source[...]
        for copy in copies:
            copy.wait_recv()
        for k in range(count - 1):
            total = total + others[k]
        return total, copies

    total, copies_x = reduce(nx_dev, my_x, "xln", mine.at[0], others_x, xs_sem, xr_sem)
    mine[1] = total
    total, copies_i = reduce(ni_dev, my_i, "inl", mine.at[1], others_i, is_sem, ir_sem)
    at = 2 * lax.broadcasted_iota(jnp.int32, (2, 2), 0) + lax.broadcasted_iota(jnp.int32, (2, 2), 1)
    result = jnp.zeros((2, 2), jnp.float32)
    for k in range(4):
        result = jnp.where(at == k, jnp.sum(total[k : k + 1], keepdims=True), result)
    norms[...] = jnp.sqrt(result)

    for copy in copies_x + copies_i:
        copy.wait_send()
    for copy, can_send in sent:
        @pl.when(can_send)
        def _():
            copy.wait_send()


def put_out(out_held, dual_held, norms_held, out, dual, norms, sems):
    half = out.shape[0] // 2
    pairs = [(norms_held, norms)]
    for at in (0, half):
        part = pl.ds(at, half)
        pairs.append((out_held.at[part], out.at[part]))
        for axis in range(3):
            pairs.append((dual_held.at[axis, part], dual.at[axis, part]))
    copies = [pltpu.make_async_copy(src, dst, sems.at[k]) for k, (src, dst) in enumerate(pairs)]
    for copy in copies:
        copy.start()
    for copy in copies:
        copy.wait()


def per_device(noisy, bound):
    ni, nx, nz = noisy.shape
    ni_dev, nx_dev = lax.axis_size("inl"), lax.axis_size("xln")
    f32 = jnp.float32
    face = pltpu.VMEM((ni, nz), f32)
    slab = pltpu.VMEM((nx, nz), f32)
    dma = pltpu.SemaphoreType.DMA
    volume = 4 * ni * nx * nz
    noisy = pltpu.with_memory_space_constraint(noisy, pltpu.HBM)
    bound = pltpu.with_memory_space_constraint(bound, pltpu.HBM)
    held = pl.pallas_call(
        functools.partial(kernel, ni_dev, nx_dev),
        out_shape=(
            pltpu.VMEM((ni, nx, nz), f32),
            pltpu.VMEM((3, ni, nx, nz), f32),
            pltpu.VMEM((2, 2), f32),
        ),
        in_specs=[pl.BlockSpec(memory_space=pltpu.HBM)] * 2,
        out_specs=(
            pl.BlockSpec(memory_space=pltpu.VMEM),
            pl.BlockSpec(memory_space=pltpu.VMEM),
            pl.BlockSpec(memory_space=pltpu.VMEM),
        ),
        scratch_shapes=[
            pltpu.VMEM((ni + 2, nx, nz), f32),
            pltpu.VMEM((ni + 1, nx, nz), f32),
            pltpu.VMEM((ni + 2, nx, nz), f32),
            slab,
            *([face] * 12),
            slab,
            pltpu.VMEM((2, 4, 128), f32),
            pltpu.VMEM((nx_dev - 1, 4, 128), f32),
            pltpu.VMEM((ni_dev - 1, 4, 128), f32),
            dma((5,)), dma((10,)), dma((10,)),
            dma((nx_dev - 1,)), dma((nx_dev - 1,)), dma((ni_dev - 1,)), dma((ni_dev - 1,)),
        ],
        compiler_params=pltpu.CompilerParams(
            collective_id=0, has_side_effects=True, vmem_limit_bytes=24 * 1024 * 1024
        ),
        cost_estimate=pl.CostEstimate(
            flops=80 * ni * nx * nz, bytes_accessed=6 * volume, transcendentals=0
        ),
        name="denoise",
    )(noisy, bound)
    in_vmem = pl.BlockSpec(memory_space=pltpu.VMEM)
    in_hbm = pl.BlockSpec(memory_space=pltpu.HBM)
    return pl.pallas_call(
        put_out,
        out_shape=(
            jax.ShapeDtypeStruct((ni, nx, nz), f32),
            jax.ShapeDtypeStruct((3, ni, nx, nz), f32),
            jax.ShapeDtypeStruct((2, 2), f32),
        ),
        in_specs=[in_vmem] * 3,
        out_specs=(in_hbm,) * 3,
        scratch_shapes=[dma((9,))],
        compiler_params=pltpu.CompilerParams(vmem_limit_bytes=1024 * 1024),
        cost_estimate=pl.CostEstimate(flops=0, bytes_accessed=4 * volume, transcendentals=0),
        name="put_out",
    )(*held)


def solution(mesh):
    in_specs = (P("inl", "xln", None), P("inl", "xln", None))
    out_specs = (P("inl", "xln", None), P(None, "inl", "xln", None), P())
    return jax.shard_map(
        per_device, mesh=mesh, in_specs=in_specs, out_specs=out_specs, check_vma=False
    )
```

```python
import functools

import jax
import jax.numpy as jnp
from jax import lax
from jax.experimental import pallas as pl
from jax.experimental.pallas import tpu as pltpu
from jax.sharding import PartitionSpec as P

SIGMA = 0.28
TAU = 0.28
GAIN = TAU / (1.0 + TAU)


def clip(value, limit):
    return jnp.minimum(jnp.maximum(value, -limit), limit)


def fold(square):
    rows, lanes = square.shape
    total = square[0:8]
    for at in range(8, rows, 8):
        total = total + square[at : at + 8]
    part = total[:, 0:128]
    for at in range(128, lanes, 128):
        part = part + total[:, at : at + 128]
    return part


def greeted(axis, count):
    return [k for k in range(1, count) if axis == "xln" or count > 4 or k in (1, count - 1)]


def split(value, dim, size):
    return [lax.slice_in_dim(value, at, at + size, axis=dim) for at in range(0, value.shape[dim], size)]


def ahead(value, dim):
    size = (8, 128)[dim]
    parts = split(value, dim, size)
    turned = [pltpu.roll(part, size - 1, dim) for part in parts]
    edge = lax.broadcasted_iota(jnp.int32, parts[0].shape, dim) == size - 1
    after = turned[1:] + [parts[-1]]
    return jnp.concatenate([jnp.where(edge, a, t) for a, t in zip(after, turned)], axis=dim)


def behind(value, dim):
    size = (8, 128)[dim]
    turned = [pltpu.roll(part, 1, dim) for part in split(value, dim, size)]
    edge = lax.broadcasted_iota(jnp.int32, turned[0].shape, dim) == 0
    before = [jnp.zeros_like(turned[0])] + turned[:-1]
    return jnp.concatenate([jnp.where(edge, a, t) for a, t in zip(before, turned)], axis=dim)


def kernel(
    ni_dev, nx_dev,
    noisy, bound, out, dual, norms,
    n, b, v, step,
    nx_first, nx_last, bx_last, nx_next, nx_prev, bx_prev,
    vx_first, vx_last, vx_next, vx_prev, dx_prev, dx_edge, di_prev,
    mine, others_x, others_i,
    load_sem, send_sem, recv_sem, xs_sem, xr_sem, is_sem, ir_sem,
):
    ni, nx, nz = noisy.shape
    top, end = ni, ni + 1
    my_i, my_x = lax.axis_index("inl"), lax.axis_index("xln")

    loads = []

    def load(src, dst):
        copy = pltpu.make_async_copy(src, dst, load_sem.at[len(loads)])
        copy.start()
        loads.append(copy)

    load(noisy.at[pl.ds(ni - 1, 1)], n.at[pl.ds(top, 1)])
    load(bound.at[pl.ds(ni - 1, 1)], b.at[pl.ds(top, 1)])
    load(noisy.at[pl.ds(0, 1)], n.at[pl.ds(1, 1)])
    load(noisy.at[pl.ds(1, ni - 2)], n.at[pl.ds(2, ni - 2)])
    load(bound.at[pl.ds(0, ni - 1)], b.at[pl.ds(1, ni - 1)])

    barrier = pltpu.get_barrier_semaphore()
    for axis, me, count in (("inl", my_i, ni_dev), ("xln", my_x, nx_dev)):
        for k in greeted(axis, count):
            pl.semaphore_signal(
                barrier, inc=1, device_id={axis: lax.rem(me + k, count)},
                device_id_type=pl.DeviceIdType.MESH,
            )
    pl.semaphore_wait(barrier, len(greeted("inl", ni_dev)) + len(greeted("xln", nx_dev)))

    sent = []

    def send(slot, src, dst, axis, forward):
        me, count = (my_i, ni_dev) if axis == "inl" else (my_x, nx_dev)
        target = lax.rem(me + (1 if forward else count - 1), count)
        copy = pltpu.make_async_remote_copy(
            src_ref=src, dst_ref=dst, send_sem=send_sem.at[slot], recv_sem=recv_sem.at[slot],
            device_id={axis: target}, device_id_type=pl.DeviceIdType.MESH,
        )
        not_last, not_first = me < count - 1, me > 0
        can_send, can_recv = (not_last, not_first) if forward else (not_first, not_last)

        @pl.when(can_send)
        def _():
            copy.start()

        sent.append((copy, can_send))

        def arrive(fill):
            @pl.when(can_recv)
            def _():
                copy.wait_recv()

            @pl.when(jnp.logical_not(can_recv))
            def _():
                fill()

        return arrive

    def setter(dst, src):
        def fill():
            dst[...] = src[...]

        return fill

    loads[0].wait()
    got_n_prev = send(0, n.at[top], n.at[0], "inl", True)
    loads[1].wait()
    got_b_prev = send(1, b.at[top], b.at[0], "inl", True)
    loads[2].wait()
    got_n_next = send(2, n.at[1], n.at[end], "inl", False)
    loads[3].wait()
    nx_last[...] = n[1:end, nx - 1, :]
    got_nx_prev = send(3, nx_last, nx_prev, "xln", True)
    nx_first[...] = n[1:end, 0, :]
    got_nx_next = send(5, nx_first, nx_next, "xln", False)
    loads[4].wait()
    bx_last[...] = b[1:end, nx - 1, :]
    got_bx_prev = send(4, bx_last, bx_prev, "xln", True)

    step[...] = jnp.zeros_like(step)

    def squares(oi, ox, oz):
        return fold(oi * oi + ox * ox + oz * oz)

    def pass_one(i, d1):
        here, limit = n[i + 1], b[i + 1]
        di = clip(SIGMA * (n[i + 2] - here), limit)
        dx = clip(SIGMA * (ahead(here, 0) - here), limit)
        dz = clip(SIGMA * (ahead(here, 1) - here), limit)
        dual[0, i] = di
        dual[1, i] = dx
        dual[2, i] = dz
        div = di - step[...]
        div = div + (dx - behind(dx, 0))
        div = div + (dz - behind(dz, 1))
        step[...] = di
        v[i + 1] = here + (2.0 * GAIN) * div
        return d1 + squares(di, dx, dz)

    zero = jnp.zeros((8, 128), jnp.float32)
    d1 = lax.fori_loop(0, ni - 1, pass_one, zero)
    here, limit = n[top], b[top]
    dx = clip(SIGMA * (ahead(here, 0) - here), limit)
    dz = clip(SIGMA * (ahead(here, 1) - here), limit)
    dual[1, ni - 1] = dx
    dual[2, ni - 1] = dz
    div = (dx - behind(dx, 0)) - step[...]
    div = div + (dz - behind(dz, 1))
    v[top] = here + (2.0 * GAIN) * div
    d1 = d1 + fold(dx * dx + dz * dz)

    got_nx_prev(setter(nx_prev, nx_first))
    got_bx_prev(setter(bx_prev, bx_last))
    got_nx_next(setter(nx_next, nx_last))
    dx_last = clip(SIGMA * (nx_next[...] - nx_last[...]), bx_last[...])
    dxp = clip(SIGMA * (nx_first[...] - nx_prev[...]), bx_prev[...])
    dual[1, :, nx - 1, :] = dx_last
    dx_prev[...] = dxp
    dx_edge[...] = dx_last
    v[1:end, nx - 1, :] = v[1:end, nx - 1, :] + (2.0 * GAIN) * dx_last
    v[1:end, 0, :] = v[1:end, 0, :] - (2.0 * GAIN) * dxp

    got_n_prev(setter(n.at[0], n.at[1]))
    got_b_prev(setter(b.at[0], b.at[1]))
    got_n_next(setter(n.at[end], n.at[top]))
    di_last = clip(SIGMA * (n[end] - n[top]), b[top])
    dip = clip(SIGMA * (n[1] - n[0]), b[0])
    dual[0, ni - 1] = di_last
    di_prev[...] = dip
    v[top] = v[top] + (2.0 * GAIN) * di_last
    v[1] = v[1] - (2.0 * GAIN) * dip
    got_v_prev = send(6, v.at[top], v.at[0], "inl", True)
    got_v_next = send(7, v.at[1], v.at[end], "inl", False)
    vx_last[...] = v[1:end, nx - 1, :]
    got_vx_prev = send(8, vx_last, vx_prev, "xln", True)
    vx_first[...] = v[1:end, 0, :]
    got_vx_next = send(9, vx_first, vx_next, "xln", False)
    d1 = d1 + fold(di_last * di_last) + fold(dx_last * dx_last)

    row = lax.broadcasted_iota(jnp.int32, (8, nz), 0)

    def inner_rows(value):
        parts = split(value, 0, 8)
        parts[0] = jnp.where(row == 0, 0.0, parts[0])
        parts[-1] = jnp.where(row == 7, 0.0, parts[-1])
        return jnp.concatenate(parts, axis=0)

    def pass_two(i, sums):
        p1, p2, d2 = sums
        here, limit, base = v[i + 1], b[i + 1], n[i + 1]
        oi, ox, oz = dual[0, i], dual[1, i], dual[2, i]
        di = clip(oi + SIGMA * (v[i + 2] - here), limit)
        dx = clip(ox + SIGMA * (ahead(here, 0) - here), limit)
        dz = clip(oz + SIGMA * (ahead(here, 1) - here), limit)
        dual[0, i] = di
        dual[1, i] = dx
        dual[2, i] = dz
        div = di - step[...]
        div = div + (dx - behind(dx, 0))
        div = div + (dz - behind(dz, 1))
        step[...] = di
        half = 0.5 * (here - base)
        change = GAIN * (div - half)
        out[i] = base + half + change
        inner = inner_rows(change)
        return (
            p1 + fold(half * half),
            p2 + fold(inner * inner),
            d2 + squares(di - oi, dx - ox, dz - oz),
        )

    step[...] = clip(dual[0, 0] + SIGMA * (v[2] - v[1]), b[1])
    sums = lax.fori_loop(1, ni - 1, pass_two, (zero,) * 3)

    got_v_next(setter(v.at[end], v.at[top]))
    sums = pass_two(ni - 1, sums)
    got_v_prev(setter(v.at[0], v.at[1]))
    step[...] = clip(di_prev[...] + SIGMA * (v[1] - v[0]), b[0])
    p1, p2, d2 = pass_two(0, sums)

    got_vx_prev(setter(vx_prev, vx_first))
    got_vx_next(setter(vx_next, vx_last))
    was = dx_edge[...]
    dx_last = clip(was + SIGMA * (vx_next[...] - vx_last[...]), bx_last[...])
    dual[1, :, nx - 1, :] = dx_last
    moved = dx_last - was
    d2 = d2 + fold(moved * moved)
    u_last = out[:, nx - 1, :] + GAIN * moved
    out[:, nx - 1, :] = u_last
    dxp = clip(dx_prev[...] + SIGMA * (vx_first[...] - vx_prev[...]), bx_prev[...])
    u_first = out[:, 0, :] - GAIN * dxp
    out[:, 0, :] = u_first
    change = u_last - (nx_last[...] + 0.5 * (vx_last[...] - nx_last[...]))
    p2 = p2 + fold(change * change)
    change = u_first - (nx_first[...] + 0.5 * (vx_first[...] - nx_first[...]))
    p2 = p2 + fold(change * change)

    for k, part in enumerate((p1, d1, p2, d2)):
        mine[0, k : k + 1] = jnp.sum(part, axis=0, keepdims=True)

    def reduce(count, me, axis, source, others, ss, rs):
        copies = []
        for k in range(1, count):
            copy = pltpu.make_async_remote_copy(
                src_ref=source, dst_ref=others.at[k - 1],
                send_sem=ss.at[k - 1], recv_sem=rs.at[k - 1],
                device_id={axis: lax.rem(me + k, count)}, device_id_type=pl.DeviceIdType.MESH,
            )
            copy.start()
            copies.append(copy)
        total = source[...]
        for copy in copies:
            copy.wait_recv()
        for k in range(count - 1):
            total = total + others[k]
        return total, copies

    total, copies_x = reduce(nx_dev, my_x, "xln", mine.at[0], others_x, xs_sem, xr_sem)
    mine[1] = total
    total, copies_i = reduce(ni_dev, my_i, "inl", mine.at[1], others_i, is_sem, ir_sem)
    at = 2 * lax.broadcasted_iota(jnp.int32, (2, 2), 0) + lax.broadcasted_iota(jnp.int32, (2, 2), 1)
    result = jnp.zeros((2, 2), jnp.float32)
    for k in range(4):
        result = jnp.where(at == k, jnp.sum(total[k : k + 1], keepdims=True), result)
    norms[...] = jnp.sqrt(result)

    for copy in copies_x + copies_i:
        copy.wait_send()
    for copy, can_send in sent:
        @pl.when(can_send)
        def _():
            copy.wait_send()


def put_out(out_held, dual_held, norms_held, out, dual, norms, sems):
    half = out.shape[0] // 2
    pairs = [(norms_held, norms)]
    for at in (0, half):
        part = pl.ds(at, half)
        pairs.append((out_held.at[part], out.at[part]))
        for axis in range(3):
            pairs.append((dual_held.at[axis, part], dual.at[axis, part]))
    copies = [pltpu.make_async_copy(src, dst, sems.at[k]) for k, (src, dst) in enumerate(pairs)]
    for copy in copies:
        copy.start()
    for copy in copies:
        copy.wait()


def per_device(noisy, bound):
    ni, nx, nz = noisy.shape
    ni_dev, nx_dev = lax.axis_size("inl"), lax.axis_size("xln")
    f32 = jnp.float32
    face = pltpu.VMEM((ni, nz), f32)
    slab = pltpu.VMEM((nx, nz), f32)
    dma = pltpu.SemaphoreType.DMA
    volume = 4 * ni * nx * nz
    noisy = pltpu.with_memory_space_constraint(noisy, pltpu.HBM)
    bound = pltpu.with_memory_space_constraint(bound, pltpu.HBM)
    held = pl.pallas_call(
        functools.partial(kernel, ni_dev, nx_dev),
        out_shape=(
            pltpu.VMEM((ni, nx, nz), f32),
            pltpu.VMEM((3, ni, nx, nz), f32),
            pltpu.VMEM((2, 2), f32),
        ),
        in_specs=[pl.BlockSpec(memory_space=pltpu.HBM)] * 2,
        out_specs=(
            pl.BlockSpec(memory_space=pltpu.VMEM),
            pl.BlockSpec(memory_space=pltpu.VMEM),
            pl.BlockSpec(memory_space=pltpu.VMEM),
        ),
        scratch_shapes=[
            pltpu.VMEM((ni + 2, nx, nz), f32),
            pltpu.VMEM((ni + 1, nx, nz), f32),
            pltpu.VMEM((ni + 2, nx, nz), f32),
            slab,
            *([face] * 12),
            slab,
            pltpu.VMEM((2, 4, 128), f32),
            pltpu.VMEM((nx_dev - 1, 4, 128), f32),
            pltpu.VMEM((ni_dev - 1, 4, 128), f32),
            dma((5,)), dma((10,)), dma((10,)),
            dma((nx_dev - 1,)), dma((nx_dev - 1,)), dma((ni_dev - 1,)), dma((ni_dev - 1,)),
        ],
        compiler_params=pltpu.CompilerParams(
            collective_id=0, has_side_effects=True, vmem_limit_bytes=24 * 1024 * 1024
        ),
        cost_estimate=pl.CostEstimate(
            flops=80 * ni * nx * nz, bytes_accessed=6 * volume, transcendentals=0
        ),
        name="denoise",
    )(noisy, bound)
    in_vmem = pl.BlockSpec(memory_space=pltpu.VMEM)
    in_hbm = pl.BlockSpec(memory_space=pltpu.HBM)
    return pl.pallas_call(
        put_out,
        out_shape=(
            jax.ShapeDtypeStruct((ni, nx, nz), f32),
            jax.ShapeDtypeStruct((3, ni, nx, nz), f32),
            jax.ShapeDtypeStruct((2, 2), f32),
        ),
        in_specs=[in_vmem] * 3,
        out_specs=(in_hbm,) * 3,
        scratch_shapes=[dma((9,))],
        compiler_params=pltpu.CompilerParams(vmem_limit_bytes=1024 * 1024),
        cost_estimate=pl.CostEstimate(flops=0, bytes_accessed=4 * volume, transcendentals=0),
        name="put_out",
    )(*held)


def solution(mesh):
    in_specs = (P("inl", "xln", None), P("inl", "xln", None))
    out_specs = (P("inl", "xln", None), P(None, "inl", "xln", None), P())
    return jax.shard_map(
        per_device, mesh=mesh, in_specs=in_specs, out_specs=out_specs, check_vma=False
    )
```

```python
import functools

import jax
import jax.numpy as jnp
from jax import lax
from jax.experimental import pallas as pl
from jax.experimental.pallas import tpu as pltpu
from jax.sharding import PartitionSpec as P

SIGMA = 0.28
TAU = 0.28
GAIN = TAU / (1.0 + TAU)


def clip(value, limit):
    return jnp.minimum(jnp.maximum(value, -limit), limit)


def fold(square):
    rows, lanes = square.shape
    total = square[0:8]
    for at in range(8, rows, 8):
        total = total + square[at : at + 8]
    part = total[:, 0:128]
    for at in range(128, lanes, 128):
        part = part + total[:, at : at + 128]
    return part


def greeted(axis, count):
    return [k for k in range(1, count) if axis == "xln" or count > 4 or k in (1, count - 1)]


def split(value, dim, size):
    return [lax.slice_in_dim(value, at, at + size, axis=dim) for at in range(0, value.shape[dim], size)]


def ahead(value, dim):
    size = (8, 128)[dim]
    parts = split(value, dim, size)
    turned = [pltpu.roll(part, size - 1, dim) for part in parts]
    edge = lax.broadcasted_iota(jnp.int32, parts[0].shape, dim) == size - 1
    after = turned[1:] + [parts[-1]]
    return jnp.concatenate([jnp.where(edge, a, t) for a, t in zip(after, turned)], axis=dim)


def behind(value, dim):
    size = (8, 128)[dim]
    turned = [pltpu.roll(part, 1, dim) for part in split(value, dim, size)]
    edge = lax.broadcasted_iota(jnp.int32, turned[0].shape, dim) == 0
    before = [jnp.zeros_like(turned[0])] + turned[:-1]
    return jnp.concatenate([jnp.where(edge, a, t) for a, t in zip(before, turned)], axis=dim)


def kernel(
    ni_dev, nx_dev,
    noisy, bound, out, dual, norms,
    n, b, v, step,
    nx_first, nx_last, bx_last, nx_next, nx_prev, bx_prev,
    vx_first, vx_last, vx_next, vx_prev, dx_prev, dx_edge, di_prev,
    mine, others_x, others_i,
    load_sem, send_sem, recv_sem, xs_sem, xr_sem, is_sem, ir_sem,
):
    ni, nx, nz = noisy.shape
    top, end = ni, ni + 1
    my_i, my_x = lax.axis_index("inl"), lax.axis_index("xln")

    loads = []

    def load(src, dst):
        copy = pltpu.make_async_copy(src, dst, load_sem.at[len(loads)])
        copy.start()
        loads.append(copy)

    load(noisy.at[pl.ds(ni - 1, 1)], n.at[pl.ds(top, 1)])
    load(bound.at[pl.ds(ni - 1, 1)], b.at[pl.ds(top, 1)])
    load(noisy.at[pl.ds(0, 1)], n.at[pl.ds(1, 1)])
    load(noisy.at[pl.ds(1, ni - 2)], n.at[pl.ds(2, ni - 2)])
    load(bound.at[pl.ds(0, ni - 1)], b.at[pl.ds(1, ni - 1)])

    barrier = pltpu.get_barrier_semaphore()
    for axis, me, count in (("inl", my_i, ni_dev), ("xln", my_x, nx_dev)):
        for k in greeted(axis, count):
            pl.semaphore_signal(
                barrier, inc=1, device_id={axis: lax.rem(me + k, count)},
                device_id_type=pl.DeviceIdType.MESH,
            )
    pl.semaphore_wait(barrier, len(greeted("inl", ni_dev)) + len(greeted("xln", nx_dev)))

    sent = []

    def send(slot, src, dst, axis, forward):
        me, count = (my_i, ni_dev) if axis == "inl" else (my_x, nx_dev)
        target = lax.rem(me + (1 if forward else count - 1), count)
        copy = pltpu.make_async_remote_copy(
            src_ref=src, dst_ref=dst, send_sem=send_sem.at[slot], recv_sem=recv_sem.at[slot],
            device_id={axis: target}, device_id_type=pl.DeviceIdType.MESH,
        )
        not_last, not_first = me < count - 1, me > 0
        can_send, can_recv = (not_last, not_first) if forward else (not_first, not_last)

        @pl.when(can_send)
        def _():
            copy.start()

        sent.append((copy, can_send))

        def arrive(fill):
            @pl.when(can_recv)
            def _():
                copy.wait_recv()

            @pl.when(jnp.logical_not(can_recv))
            def _():
                fill()

        return arrive

    def setter(dst, src):
        def fill():
            dst[...] = src[...]

        return fill

    loads[0].wait()
    got_n_prev = send(0, n.at[top], n.at[0], "inl", True)
    loads[1].wait()
    got_b_prev = send(1, b.at[top], b.at[0], "inl", True)
    loads[2].wait()
    got_n_next = send(2, n.at[1], n.at[end], "inl", False)
    loads[3].wait()
    nx_last[...] = n[1:end, nx - 1, :]
    got_nx_prev = send(3, nx_last, nx_prev, "xln", True)
    nx_first[...] = n[1:end, 0, :]
    got_nx_next = send(5, nx_first, nx_next, "xln", False)
    loads[4].wait()
    bx_last[...] = b[1:end, nx - 1, :]
    got_bx_prev = send(4, bx_last, bx_prev, "xln", True)

    step[...] = jnp.zeros_like(step)

    def squares(oi, ox, oz):
        return fold(oi * oi + ox * ox + oz * oz)

    def pass_one(i, d1):
        here, limit = n[i + 1], b[i + 1]
        di = clip(SIGMA * (n[i + 2] - here), limit)
        dx = clip(SIGMA * (ahead(here, 0) - here), limit)
        dz = clip(SIGMA * (ahead(here, 1) - here), limit)
        dual[0, i] = di
        dual[1, i] = dx
        dual[2, i] = dz
        div = di - step[...]
        div = div + (dx - behind(dx, 0))
        div = div + (dz - behind(dz, 1))
        step[...] = di
        v[i + 1] = here + (2.0 * GAIN) * div
        return d1 + squares(di, dx, dz)

    zero = jnp.zeros((8, 128), jnp.float32)
    d1 = lax.fori_loop(0, ni - 1, pass_one, zero)
    here, limit = n[top], b[top]
    dx = clip(SIGMA * (ahead(here, 0) - here), limit)
    dz = clip(SIGMA * (ahead(here, 1) - here), limit)
    dual[1, ni - 1] = dx
    dual[2, ni - 1] = dz
    div = (dx - behind(dx, 0)) - step[...]
    div = div + (dz - behind(dz, 1))
    v[top] = here + (2.0 * GAIN) * div
    d1 = d1 + fold(dx * dx + dz * dz)

    got_nx_prev(setter(nx_prev, nx_first))
    got_bx_prev(setter(bx_prev, bx_last))
    got_nx_next(setter(nx_next, nx_last))
    dx_last = clip(SIGMA * (nx_next[...] - nx_last[...]), bx_last[...])
    dxp = clip(SIGMA * (nx_first[...] - nx_prev[...]), bx_prev[...])
    dual[1, :, nx - 1, :] = dx_last
    dx_prev[...] = dxp
    dx_edge[...] = dx_last
    v[1:end, nx - 1, :] = v[1:end, nx - 1, :] + (2.0 * GAIN) * dx_last
    v[1:end, 0, :] = v[1:end, 0, :] - (2.0 * GAIN) * dxp

    got_n_prev(setter(n.at[0], n.at[1]))
    got_b_prev(setter(b.at[0], b.at[1]))
    got_n_next(setter(n.at[end], n.at[top]))
    di_last = clip(SIGMA * (n[end] - n[top]), b[top])
    dip = clip(SIGMA * (n[1] - n[0]), b[0])
    dual[0, ni - 1] = di_last
    di_prev[...] = dip
    v[top] = v[top] + (2.0 * GAIN) * di_last
    v[1] = v[1] - (2.0 * GAIN) * dip
    got_v_prev = send(6, v.at[top], v.at[0], "inl", True)
    got_v_next = send(7, v.at[1], v.at[end], "inl", False)
    vx_last[...] = v[1:end, nx - 1, :]
    got_vx_prev = send(8, vx_last, vx_prev, "xln", True)
    vx_first[...] = v[1:end, 0, :]
    got_vx_next = send(9, vx_first, vx_next, "xln", False)
    d1 = d1 + fold(di_last * di_last) + fold(dx_last * dx_last)

    row = lax.broadcasted_iota(jnp.int32, (8, nz), 0)

    def inner_rows(value):
        parts = split(value, 0, 8)
        parts[0] = jnp.where(row == 0, 0.0, parts[0])
        parts[-1] = jnp.where(row == 7, 0.0, parts[-1])
        return jnp.concatenate(parts, axis=0)

    def pass_two(i, sums):
        p1, p2, d2 = sums
        here, limit, base = v[i + 1], b[i + 1], n[i + 1]
        oi, ox, oz = dual[0, i], dual[1, i], dual[2, i]
        di = clip(oi + SIGMA * (v[i + 2] - here), limit)
        dx = clip(ox + SIGMA * (ahead(here, 0) - here), limit)
        dz = clip(oz + SIGMA * (ahead(here, 1) - here), limit)
        dual[0, i] = di
        dual[1, i] = dx
        dual[2, i] = dz
        div = di - step[...]
        div = div + (dx - behind(dx, 0))
        div = div + (dz - behind(dz, 1))
        step[...] = di
        half = 0.5 * (here - base)
        change = GAIN * (div - half)
        out[i] = base + half + change
        inner = inner_rows(change)
        return (
            p1 + fold(half * half),
            p2 + fold(inner * inner),
            d2 + squares(di - oi, dx - ox, dz - oz),
        )

    step[...] = clip(dual[0, 0] + SIGMA * (v[2] - v[1]), b[1])
    sums = lax.fori_loop(1, ni - 1, pass_two, (zero,) * 3)

    got_v_next(setter(v.at[end], v.at[top]))
    sums = pass_two(ni - 1, sums)
    got_v_prev(setter(v.at[0], v.at[1]))
    step[...] = clip(di_prev[...] + SIGMA * (v[1] - v[0]), b[0])
    p1, p2, d2 = pass_two(0, sums)

    got_vx_prev(setter(vx_prev, vx_first))
    got_vx_next(setter(vx_next, vx_last))
    was = dx_edge[...]
    dx_last = clip(was + SIGMA * (vx_next[...] - vx_last[...]), bx_last[...])
    dual[1, :, nx - 1, :] = dx_last
    moved = dx_last - was
    d2 = d2 + fold(moved * moved)
    u_last = out[:, nx - 1, :] + GAIN * moved
    out[:, nx - 1, :] = u_last
    dxp = clip(dx_prev[...] + SIGMA * (vx_first[...] - vx_prev[...]), bx_prev[...])
    u_first = out[:, 0, :] - GAIN * dxp
    out[:, 0, :] = u_first
    change = u_last - (nx_last[...] + 0.5 * (vx_last[...] - nx_last[...]))
    p2 = p2 + fold(change * change)
    change = u_first - (nx_first[...] + 0.5 * (vx_first[...] - nx_first[...]))
    p2 = p2 + fold(change * change)

    for k, part in enumerate((p1, d1, p2, d2)):
        mine[0, k : k + 1] = jnp.sum(part, axis=0, keepdims=True)

    def reduce(count, me, axis, source, others, ss, rs):
        copies = []
        for k in range(1, count):
            copy = pltpu.make_async_remote_copy(
                src_ref=source, dst_ref=others.at[k - 1],
                send_sem=ss.at[k - 1], recv_sem=rs.at[k - 1],
                device_id={axis: lax.rem(me + k, count)}, device_id_type=pl.DeviceIdType.MESH,
            )
            copy.start()
            copies.append(copy)
        total = source[...]
        for copy in copies:
            copy.wait_recv()
        for k in range(count - 1):
            total = total + others[k]
        return total, copies

    total, copies_x = reduce(nx_dev, my_x, "xln", mine.at[0], others_x, xs_sem, xr_sem)
    mine[1] = total
    total, copies_i = reduce(ni_dev, my_i, "inl", mine.at[1], others_i, is_sem, ir_sem)
    at = 2 * lax.broadcasted_iota(jnp.int32, (2, 2), 0) + lax.broadcasted_iota(jnp.int32, (2, 2), 1)
    result = jnp.zeros((2, 2), jnp.float32)
    for k in range(4):
        result = jnp.where(at == k, jnp.sum(total[k : k + 1], keepdims=True), result)
    norms[...] = jnp.sqrt(result)

    for copy in copies_x + copies_i:
        copy.wait_send()
    for copy, can_send in sent:
        @pl.when(can_send)
        def _():
            copy.wait_send()


def put_out(out_held, dual_held, norms_held, out, dual, norms, sems):
    size = out.shape[0] // 4
    pairs = [(norms_held, norms)]
    for at in range(0, out.shape[0], size):
        part = pl.ds(at, size)
        pairs.append((out_held.at[part], out.at[part]))
        for axis in range(3):
            pairs.append((dual_held.at[axis, part], dual.at[axis, part]))
    copies = [pltpu.make_async_copy(src, dst, sems.at[k]) for k, (src, dst) in enumerate(pairs)]
    for k, copy in enumerate(copies):
        copy.start(priority=k % 2)
    for copy in copies:
        copy.wait()


def per_device(noisy, bound):
    ni, nx, nz = noisy.shape
    ni_dev, nx_dev = lax.axis_size("inl"), lax.axis_size("xln")
    f32 = jnp.float32
    face = pltpu.VMEM((ni, nz), f32)
    slab = pltpu.VMEM((nx, nz), f32)
    dma = pltpu.SemaphoreType.DMA
    volume = 4 * ni * nx * nz
    noisy = pltpu.with_memory_space_constraint(noisy, pltpu.HBM)
    bound = pltpu.with_memory_space_constraint(bound, pltpu.HBM)
    held = pl.pallas_call(
        functools.partial(kernel, ni_dev, nx_dev),
        out_shape=(
            pltpu.VMEM((ni, nx, nz), f32),
            pltpu.VMEM((3, ni, nx, nz), f32),
            pltpu.VMEM((2, 2), f32),
        ),
        in_specs=[pl.BlockSpec(memory_space=pltpu.HBM)] * 2,
        out_specs=(
            pl.BlockSpec(memory_space=pltpu.VMEM),
            pl.BlockSpec(memory_space=pltpu.VMEM),
            pl.BlockSpec(memory_space=pltpu.VMEM),
        ),
        scratch_shapes=[
            pltpu.VMEM((ni + 2, nx, nz), f32),
            pltpu.VMEM((ni + 1, nx, nz), f32),
            pltpu.VMEM((ni + 2, nx, nz), f32),
            slab,
            *([face] * 12),
            slab,
            pltpu.VMEM((2, 4, 128), f32),
            pltpu.VMEM((nx_dev - 1, 4, 128), f32),
            pltpu.VMEM((ni_dev - 1, 4, 128), f32),
            dma((5,)), dma((10,)), dma((10,)),
            dma((nx_dev - 1,)), dma((nx_dev - 1,)), dma((ni_dev - 1,)), dma((ni_dev - 1,)),
        ],
        compiler_params=pltpu.CompilerParams(
            collective_id=0, has_side_effects=True, vmem_limit_bytes=24 * 1024 * 1024
        ),
        cost_estimate=pl.CostEstimate(
            flops=80 * ni * nx * nz, bytes_accessed=6 * volume, transcendentals=0
        ),
        name="denoise",
    )(noisy, bound)
    in_vmem = pl.BlockSpec(memory_space=pltpu.VMEM)
    in_hbm = pl.BlockSpec(memory_space=pltpu.HBM)
    return pl.pallas_call(
        put_out,
        out_shape=(
            jax.ShapeDtypeStruct((ni, nx, nz), f32),
            jax.ShapeDtypeStruct((3, ni, nx, nz), f32),
            jax.ShapeDtypeStruct((2, 2), f32),
        ),
        in_specs=[in_vmem] * 3,
        out_specs=(in_hbm,) * 3,
        scratch_shapes=[dma((17,))],
        compiler_params=pltpu.CompilerParams(vmem_limit_bytes=1024 * 1024),
        cost_estimate=pl.CostEstimate(flops=0, bytes_accessed=4 * volume, transcendentals=0),
        name="put_out",
    )(*held)


def solution(mesh):
    in_specs = (P("inl", "xln", None), P("inl", "xln", None))
    out_specs = (P("inl", "xln", None), P(None, "inl", "xln", None), P())
    return jax.shard_map(
        per_device, mesh=mesh, in_specs=in_specs, out_specs=out_specs, check_vma=False
    )
```
